512 devices in a mesh: groups: 2 (over y), seq: 16 (over z), exp: 8 (over x), tp: 2 (over core).
Axes of the slice: x: 8, y: 2, z: 16, core: 2. Of those that a mesh axis runs over, the one named last changes fastest.
The devices are a block of a 8x8x16 slice.
Arguments:
- attn_query: bfloat16 [8192, 1152], P(('groups', 'seq'), ('exp', 'tp')), parts along dimension 0, may hold values from -6 to 6
- fresh_keys: bfloat16 [8192, 1152], P(('groups', 'seq'), ('exp', 'tp')), parts along dimension 0, may hold values from -6 to 6
- fresh_values: bfloat16 [8192, 1152], P(('groups', 'seq'), ('exp', 'tp')), parts along dimension 0, may hold values from -6 to 6
- stale_keys: bfloat16 [8192, 1152], P(('groups', 'seq'), ('exp', 'tp')), parts along dimension 0, may hold values from -6 to 6
- stale_values: bfloat16 [8192, 1152], P(('groups', 'seq'), ('exp', 'tp')), parts along dimension 0, may hold values from -6 to 6
- block_flags: int32 [64], P(('groups', 'seq')), parts along dimension 0, may hold values 0 or 1
- moe_tokens: bfloat16 [65536, 1152], P(('groups', 'seq', 'exp', 'tp')), parts along dimension 0, may hold values from -6 to 6
- expert_ids: int32 [65536, 2], P(('groups', 'seq', 'exp', 'tp')), parts along dimension 0, may hold values from 0 to 15, all different within a row; in each aligned block of 128 rows (0 to 127, 128 to 255, ...) at most 20 rows name the same one
- gate_weights: float32 [65536, 2], P(('groups', 'seq', 'exp', 'tp')), parts along dimension 0, may hold values from 0.25 to 1
- up_weight: bfloat16 [16, 1152, 4608], P('seq', None, ('exp', 'tp')), may hold values from -0.1875 to 0.1875
- up_bias: float32 [16, 4608], P('seq', ('exp', 'tp')), may hold values from -3 to 3
- down_weight: bfloat16 [16, 4608, 1152], P('seq', ('exp', 'tp')), may hold values from -0.09375 to 0.09375
- down_bias: float32 [16, 1152], P('seq'), may hold values from -2 to 2
Outputs:
- attn_out: bfloat16 [8192, 1152], P(('groups', 'seq'), ('exp', 'tp')), parts along dimension 0
- moe_out: bfloat16 [65536, 1152], P(('groups', 'seq', 'exp', 'tp')), parts along dimension 0
The draws below stay inside these ranges and needn't reach their ends.
There are 2 independent parts, one for each index of `groups`. The reference program is written for one: setup_inputs(seed, part) draws one part's arguments, and reference() takes and returns one part's arrays. A program takes and returns all parts, laid end to end along the dimension named above; an argument that names none is the same for every part. Nothing has to cross between parts.
Inputs may be any that keep to these rules, and one draw needn't show every extreme that they name: `expert_ids`: the 2 ids of a token differ. In the rows of one device no expert is named more than 20 times, and in every draw some expert is named exactly 20 times in some device's rows.
All inputs are finite; a program needn't handle non-finite values. No bound on the sum of `block_flags` on one device may be relied on, other than what follows from the above.
Results may differ from the reference program's by a relative error of at most 0.014.
Values may be sent and summed in bfloat16 or wider, within the bound.
No kernel may reach another device: no remote copies, remote signals or barrier semaphores. Data moves between devices by JAX's collectives and lax.ppermute only.
A program may use at most 64 MiB of HBM per device.

```python
import math
import jax
import jax.numpy as jnp
import numpy as np
from jax import lax

D = 1152
HEADS = 16
HD = 72
FF = 4608
TOP = 2
EXPERTS = 16
BLK = 128
TOK_DEV = 128
SEQLEN = 4096
MOE_TOK = 32768
CAP = 20


def drawn(key):
    shape = (SEQLEN, HEADS * HD)
    query = jnp.clip(jax.random.normal(jax.random.fold_in(key, 101), shape, jnp.float32), -6.0, 6.0)
    keys_new = jnp.clip(jax.random.normal(jax.random.fold_in(key, 102), shape, jnp.float32), -6.0, 6.0)
    keys_old = jnp.clip(jax.random.normal(jax.random.fold_in(key, 103), shape, jnp.float32), -6.0, 6.0)
    return (query, keys_new, keys_old)


def draw_attn_query(key, part):
    return drawn(key)[0].astype(jnp.bfloat16)


def draw_fresh_keys(key, part):
    return drawn(key)[1].astype(jnp.bfloat16)


def draw_stale_keys(key, part):
    return drawn(key)[2].astype(jnp.bfloat16)


def place_ends(values, key, smallest, high):
    spot = [jax.random.randint(jax.random.fold_in(key, axis), (), 0, length) for axis, length in enumerate(values.shape)]
    main_axis = values.shape.index(max(values.shape))
    neighbour = spot[:main_axis] + [(spot[main_axis] + 1) % values.shape[main_axis]] + spot[main_axis + 1:]
    return values.at[tuple(spot)].set(smallest).at[tuple(neighbour)].set(high)


def steps_of(key, dims, shards, smallest, top_value):
    level = 1.0
    for dim, blocks in shards:
        heights = jax.random.uniform(jax.random.fold_in(jax.random.fold_in(key, 6), dim), (blocks,), jnp.float32, smallest / len(shards), top_value / len(shards))
        level = level * jnp.repeat(jnp.exp(heights), dims[dim] // blocks).reshape((-1,) + (1,) * (len(dims) - 1 - dim))
    return level


def assign_block(rng, own, number, rows, number_of, top, limit, lean):
    ranking = jax.random.permutation(rng, number_of)
    heavy_load, ordinary = portions_of(number_of, rows * top, limit, lean, True), portions_of(number_of, rows * top, limit, lean, False)
    places = jnp.arange(number_of)

    def named(tallies, offset_by):
        used = int((tallies > 0).sum())
        fixed = max(1, used // 4)
        passed = fixed + (places - fixed + offset_by * (used - fixed)) % max(1, number_of - fixed)
        return jnp.zeros((number_of,), jnp.int32).at[ranking[jnp.where(places < fixed, places, passed)]].set(jnp.asarray(tallies, jnp.int32))

    tallies = jnp.where(number % 4 == 0, named(heavy_load, number // 4), named(ordinary, number - number // 4 - 1))
    mixed = jax.random.permutation(jax.random.fold_in(own, 3), number_of)
    giver, sink = mixed[0:number_of // 2 * 2:2], mixed[1:number_of // 2 * 2:2]
    slack = jnp.minimum(tallies[giver] - 1, limit - tallies[sink]) // 2
    slack = jnp.where((giver == ranking[0]) | (sink == ranking[0]) | (tallies[sink] == 0), 0, jnp.maximum(slack, 0))
    passed = jax.random.randint(jax.random.fold_in(own, 4), (number_of // 2,), 0, 1 << 20) % (slack + 1)
    tallies = tallies.at[giver].add(-passed).at[sink].add(passed)
    labels = jnp.searchsorted(jnp.cumsum(tallies), jnp.arange(rows * top), side="right").astype(jnp.int32)
    listing = labels.reshape(top, rows).T
    listing = listing[jax.random.permutation(jax.random.fold_in(own, 1), rows)]
    offset_by = jax.random.randint(jax.random.fold_in(own, 2), (rows, 1), 0, top)
    return jnp.take_along_axis(listing, (jnp.arange(top)[None, :] + offset_by) % top, axis=1)


def portions_of(amount, total, limit, lean, full):
    weights = [(1 << 20) // math.isqrt(grade ** lean) + 1 for grade in range(1, amount + 1)]
    largest = limit if full else min(limit, max(-(-total // amount), total * weights[0] // sum(weights)))
    least = 1 if total - largest >= amount - 1 else 0
    given, spare = [largest] + [least] * (amount - 1), total - largest - least * (amount - 1)
    while spare > 0:
        free = [i for i in range(1, amount) if given[i] < largest] or [i for i in range(1, amount) if given[i] < limit]
        whole, budget = sum([weights[i] for i in free]), spare
        for i in free:
            more = min(limit - given[i], max(1, budget * weights[i] // whole), spare)
            given[i] = given[i] + more
            spare = spare - more
    return np.array(given)


def noise(key, dims, width, limit, cuts=(), kind=jnp.bfloat16):
    values = jax.random.normal(key, dims, jnp.float32) * width
    if len(cuts) > 0:
        values = steps_of(key, dims, cuts, -0.22, 0.18) * values
    return jnp.clip(values, min=-limit, max=limit).astype(kind)


def setup_inputs(seed: int = 0, part: int = 0) -> dict:
    streams_of = jax.random.split(jax.random.key(seed), 14)
    part_splits = jax.random.split(jax.random.fold_in(streams_of[13], part), 14)
    attn_query = draw_attn_query(jax.random.fold_in(jax.random.fold_in(streams_of[13], part), 71), part)
    fresh_keys = draw_fresh_keys(jax.random.fold_in(jax.random.fold_in(streams_of[13], part), 71), part)
    fresh_values = noise(part_splits[2], (SEQLEN, HEADS * HD), 1.0, 6.0, ((0, 16), (1, 16)))
    stale_keys = draw_stale_keys(jax.random.fold_in(jax.random.fold_in(streams_of[13], part), 71), part)
    stale_values = noise(part_splits[4], (SEQLEN, HEADS * HD), 1.0, 6.0, ((0, 16), (1, 16)))
    block_flags = place_ends((jax.random.randint(part_splits[5], (SEQLEN // BLK,), 0, 2) < 1).astype(jnp.int32), jax.random.fold_in(part_splits[5], 1), 0, 1)
    moe_tokens = noise(part_splits[6], (MOE_TOK, D), 1.0, 6.0, ((0, 256),))
    expert_ids_keys = jax.random.split(jax.random.fold_in(part_splits[7], 1), MOE_TOK // TOK_DEV)
    expert_ids_turns = jax.random.permutation(jax.random.fold_in(part_splits[7], 3), MOE_TOK // TOK_DEV)
    expert_ids = jax.vmap(lambda own, number: assign_block(jax.random.fold_in(part_splits[7], 2), own, number, TOK_DEV, EXPERTS, TOP, CAP, 2))(expert_ids_keys, expert_ids_turns).reshape((MOE_TOK, TOP))
    gate_weights = jnp.clip(jnp.exp(math.log(1.0) - 1.3862944 * jax.random.uniform(part_splits[8], (MOE_TOK, TOP), jnp.float32) ** steps_of(part_splits[8], (MOE_TOK, TOP), ((0, 256),), -0.2, 0.2)), 0.25, 1.0)
    up_weight = noise(streams_of[9], (EXPERTS, D, FF), D ** -0.5, 0.1875, ((0, 16), (2, 16)))
    up_bias = noise(streams_of[10], (EXPERTS, FF), 0.5, 3.0, ((0, 16), (1, 16)), jnp.float32)
    down_weight = noise(streams_of[11], (EXPERTS, FF, D), FF ** -0.5, 0.09375, ((0, 16), (1, 16)))
    down_bias = noise(streams_of[12], (EXPERTS, D), 0.3, 2.0, ((0, 16),), jnp.float32)
    return {"attn_query": attn_query, "fresh_keys": fresh_keys, "fresh_values": fresh_values, "stale_keys": stale_keys, "stale_values": stale_values, "block_flags": block_flags, "moe_tokens": moe_tokens, "expert_ids": expert_ids, "gate_weights": gate_weights, "up_weight": up_weight, "up_bias": up_bias, "down_weight": down_weight, "down_bias": down_bias}


def attention_part(attn_query, fresh_keys, fresh_values, stale_keys, stale_values, block_flags):
    row_flags = (jnp.repeat(block_flags, BLK) == 1)[:, None]
    keys = jnp.where(row_flags, fresh_keys, stale_keys)
    values = jnp.where(row_flags, fresh_values, stale_values)
    scale = 1.0 / math.sqrt(HD)
    query_block = math.gcd(SEQLEN, 1024)

    def head_fn(head):
        first = (head * HD).astype(jnp.int32)
        head_query = lax.dynamic_slice_in_dim(attn_query, first, HD, 1)
        head_keys = lax.dynamic_slice_in_dim(keys, first, HD, 1)
        head_values = lax.dynamic_slice_in_dim(values, first, HD, 1)

        def block_fn(index):
            lead = (index * query_block).astype(jnp.int32)
            rows = lax.dynamic_slice_in_dim(head_query, lead, query_block, 0)
            scores = jnp.dot(rows, head_keys.T, preferred_element_type=jnp.float32) * scale
            highest = lax.optimization_barrier(jnp.max(scores, axis=-1, keepdims=True))
            probs = jnp.exp(scores - highest)
            totals = lax.optimization_barrier(jnp.sum(probs, axis=-1, keepdims=True))
            mixed = jnp.dot(probs.astype(jnp.bfloat16), head_values, preferred_element_type=jnp.float32) / totals
            return mixed.astype(jnp.bfloat16)
        return lax.map(block_fn, jnp.arange(SEQLEN // query_block, dtype=jnp.int32))
    heads_out = lax.map(head_fn, jnp.arange(HEADS, dtype=jnp.int32))
    heads_out = heads_out.reshape(HEADS, SEQLEN, HD)
    return jnp.transpose(heads_out, (1, 0, 2)).reshape(SEQLEN, HEADS * HD)

def expert_part(moe_tokens, expert_ids, gate_weights, up_weight, up_bias, down_weight, down_bias):
    blocks = MOE_TOK // TOK_DEV
    block_ids = expert_ids.reshape(blocks, TOP * TOK_DEV)
    hits = (block_ids[:, :, None] == jnp.arange(EXPERTS, dtype=jnp.int32)[None, None, :]).astype(jnp.int32)
    before = jnp.cumsum(hits, axis=1) - hits
    place = lax.optimization_barrier(jnp.sum(before * hits, axis=-1)).reshape(-1).astype(jnp.int32)
    flat_expert = block_ids.reshape(-1).astype(jnp.int32)
    flat_block = jnp.repeat(jnp.arange(blocks, dtype=jnp.int32), TOP * TOK_DEV)
    repeated = jnp.repeat(moe_tokens, TOP, axis=0)
    buffer = jnp.zeros((EXPERTS, blocks, CAP, D), jnp.bfloat16)
    buffer = buffer.at[flat_expert, flat_block, place].set(repeated)

    def expert_fn(operands):
        slots, w_up, b_up, w_down, b_down = operands
        rows = slots.reshape(blocks * CAP, D)
        hidden = jax.nn.gelu(jnp.dot(rows, w_up, preferred_element_type=jnp.float32) + b_up[None, :]).astype(jnp.bfloat16)
        result = jnp.dot(hidden, w_down, preferred_element_type=jnp.float32) + b_down[None, :]
        return result.astype(jnp.bfloat16).reshape(blocks, CAP, D)
    expert_y = lax.map(expert_fn, (buffer, up_weight, up_bias, down_weight, down_bias))
    picked = expert_y[flat_expert, flat_block, place].reshape(MOE_TOK, TOP, D).astype(jnp.float32)
    combined = lax.optimization_barrier(jnp.sum(picked * gate_weights[:, :, None], axis=1))
    return combined.astype(jnp.bfloat16)

def reference(attn_query, fresh_keys, fresh_values, stale_keys, stale_values, block_flags, moe_tokens, expert_ids, gate_weights, up_weight, up_bias, down_weight, down_bias):
    attn_out = attention_part(attn_query, fresh_keys, fresh_values, stale_keys, stale_values, block_flags)
    moe_out = expert_part(moe_tokens, expert_ids, gate_weights, up_weight, up_bias, down_weight, down_bias)
    return (attn_out, moe_out)
```

```python
import math

import jax
import jax.numpy as jnp
from jax import lax
from jax.sharding import PartitionSpec as P

HD = 72
TILE = 384
FIRST = 1


def shifted(value, axis, step):
    size = lax.axis_size(axis)
    return lax.ppermute(value, axis, [(i, (i + step) % size) for i in range(size)])


def ring_gather(own, axis):
    size = lax.axis_size(axis)
    arrived = [own]
    right = left = own
    for _ in range(1, (size + 1) // 2):
        right, left = shifted(right, axis, 1), shifted(left, axis, -1)
        arrived += [right, left]
    if size % 2 == 0:
        half = own.shape[0] // 16 * 8
        arrived.append(
            jnp.concatenate(
                [shifted(right[:half], axis, 1), shifted(left[half:], axis, -1)], axis=0
            )
        )
    return arrived


def spread_gather(own, axis):
    size = lax.axis_size(axis)
    near = math.gcd(size, 4)
    far = [own] + [shifted(own, axis, near * k) for k in range(1, size // near)]
    block = jnp.concatenate(far, axis=1)
    steps = [k if k <= near // 2 else k - near for k in range(1, near)]
    return [block] + [shifted(block, axis, k) for k in steps]


def attention_part(attn_query, fresh_keys, fresh_values, stale_keys, stale_values, block_flags):
    length = attn_query.shape[0]
    heads_here = attn_query.shape[1] // HD
    width = heads_here * HD
    row_flags = (jnp.repeat(block_flags, length // block_flags.shape[0]) == 1)[:, None]
    keys = jnp.where(row_flags, fresh_keys, stale_keys)
    values = jnp.where(row_flags, fresh_values, stale_values)
    own = jnp.concatenate([keys.T, values.T], axis=0)
    gathered = jnp.concatenate(spread_gather(own, "seq"), axis=1)
    scale = 1.0 / math.sqrt(HD)
    outs = []
    for head in range(heads_here):
        cols = slice(head * HD, (head + 1) * HD)
        all_keys = gathered[cols]
        all_values = gathered[width + head * HD : width + (head + 1) * HD]
        scores = (
            jnp.dot(attn_query[:, cols], all_keys, preferred_element_type=jnp.float32) * scale
        )
        highest = jnp.max(scores, axis=-1, keepdims=True)
        probs = jnp.exp(scores - highest)
        totals = jnp.sum(probs, axis=-1, keepdims=True)
        mixed = lax.dot_general(
            probs.astype(jnp.bfloat16),
            all_values,
            (((1,), (1,)), ((), ())),
            preferred_element_type=jnp.float32,
        )
        outs.append((mixed / totals).astype(jnp.bfloat16))
    return jnp.concatenate(outs, axis=1)


def expert_part(moe_tokens, expert_ids, gate_weights, up_weight, up_bias, down_weight, down_bias):
    tokens_here, width = moe_tokens.shape
    choose = expert_ids.shape[1]
    number = lax.axis_size("seq") * up_weight.shape[0]
    capacity = 5 * tokens_here // (2 * number)
    slots = number * capacity
    hidden_here = up_weight.shape[2]
    tiles = width // TILE

    def columns(value, k):
        return value[:, k * TILE : (k + 1) * TILE]

    turned = up_weight[0].T
    bias_high = up_bias[0].astype(jnp.bfloat16)
    bias_low = (up_bias[0] - bias_high.astype(jnp.float32)).astype(jnp.bfloat16)
    bias_rows = jnp.pad(jnp.stack([bias_high, bias_low]), ((0, 6), (0, TILE - hidden_here)))
    phases = [
        jnp.concatenate(
            [columns(turned, k) for k in range(tiles)]
            + [bias_rows]
            + [columns(down_weight[0], k) for k in range(FIRST)],
            axis=0,
        )
    ] + [columns(down_weight[0], k) for k in range(FIRST, tiles)]
    rings = [ring_gather(own, "exp") for own in phases]

    flat_ids = expert_ids.reshape(-1)
    pairs = flat_ids.shape[0]
    hits = (flat_ids[:, None] == jnp.arange(number, dtype=jnp.int32)[None, :]).astype(jnp.bfloat16)
    index = jnp.arange(pairs, dtype=jnp.int32)
    earlier = (index[None, :] < index[:, None]).astype(jnp.bfloat16)
    before = jnp.dot(earlier, hits, preferred_element_type=jnp.float32)
    place = jnp.sum(before * hits.astype(jnp.float32), axis=1).astype(jnp.int32)
    slot = (flat_ids * capacity + place).reshape(tokens_here, choose)
    slot_index = jnp.arange(slots, dtype=jnp.int32)
    match = slot[:, :, None] == slot_index[None, None, :]
    table = jnp.sum(match.astype(jnp.float32), axis=1).astype(jnp.bfloat16)
    gates = jnp.sum(jnp.where(match, gate_weights[:, :, None], 0.0), axis=1)
    gates_high = gates.astype(jnp.bfloat16)
    gates_low = (gates - gates_high.astype(jnp.float32)).astype(jnp.bfloat16)
    buffer = lax.dot_general(
        table, moe_tokens, (((0,), (0,)), ((), ())), preferred_element_type=jnp.float32
    ).astype(jnp.bfloat16)
    buffer = buffer.reshape(number, capacity, width)
    received = lax.all_to_all(buffer, "seq", split_axis=0, concat_axis=0, tiled=True)
    rows = received.reshape(slots, width)
    both = jnp.concatenate([rows, shifted(rows, "tp", 1)], axis=0)

    hidden = []
    for piece in rings[0]:
        bias = piece[tiles * hidden_here : tiles * hidden_here + 2, :hidden_here].astype(
            jnp.float32
        )
        weight = jnp.concatenate(
            [piece[k * hidden_here : (k + 1) * hidden_here] for k in range(tiles)], axis=1
        )
        raised = lax.dot_general(
            both, weight, (((1,), (1,)), ((), ())), preferred_element_type=jnp.float32
        )
        hidden.append(jax.nn.gelu(raised + bias[0] + bias[1]).astype(jnp.bfloat16))
    outs = []
    skip = tiles * hidden_here + bias_rows.shape[0]
    for k in range(tiles):
        if k < FIRST:
            downs = [p[skip + k * hidden_here : skip + (k + 1) * hidden_here] for p in rings[0]]
        else:
            downs = rings[1 + k - FIRST]
        total = sum(
            jnp.dot(h, d, preferred_element_type=jnp.float32) for h, d in zip(hidden, downs)
        )
        other = shifted(total[slots:].astype(jnp.bfloat16), "tp", 1)
        result = total[:slots] + other.astype(jnp.float32) + columns(down_bias, k)
        result = result.astype(jnp.bfloat16).reshape(number, capacity, TILE)
        back = lax.all_to_all(result, "seq", split_axis=0, concat_axis=0, tiled=True)
        back = back.reshape(slots, TILE)
        outs.append(
            jnp.dot(gates_high, back, preferred_element_type=jnp.float32)
            + jnp.dot(gates_low, back, preferred_element_type=jnp.float32)
        )
    return jnp.concatenate(outs, axis=1).astype(jnp.bfloat16)


def local(
    attn_query,
    fresh_keys,
    fresh_values,
    stale_keys,
    stale_values,
    block_flags,
    moe_tokens,
    expert_ids,
    gate_weights,
    up_weight,
    up_bias,
    down_weight,
    down_bias,
):
    attn_out = attention_part(
        attn_query, fresh_keys, fresh_values, stale_keys, stale_values, block_flags
    )
    moe_out = expert_part(
        moe_tokens, expert_ids, gate_weights, up_weight, up_bias, down_weight, down_bias
    )
    return (attn_out, moe_out)


def solution(mesh):
    in_specs = (
        P(("groups", "seq"), ("exp", "tp")),
        P(("groups", "seq"), ("exp", "tp")),
        P(("groups", "seq"), ("exp", "tp")),
        P(("groups", "seq"), ("exp", "tp")),
        P(("groups", "seq"), ("exp", "tp")),
        P(("groups", "seq")),
        P(("groups", "seq", "exp", "tp"), None),
        P(("groups", "seq", "exp", "tp"), None),
        P(("groups", "seq", "exp", "tp"), None),
        P("seq", None, ("exp", "tp")),
        P("seq", ("exp", "tp")),
        P("seq", ("exp", "tp"), None),
        P("seq", None),
    )
    out_specs = (P(("groups", "seq"), ("exp", "tp")), P(("groups", "seq", "exp", "tp"), None))
    return jax.shard_map(local, mesh=mesh, in_specs=in_specs, out_specs=out_specs, check_vma=False)
```

```python
import functools
import math

import jax
import jax.numpy as jnp
from jax import lax
from jax.experimental import pallas as pl
from jax.experimental.pallas import tpu as pltpu
from jax.sharding import PartitionSpec as P


HD = 72
ROWS = 8
LANES = 128
BF = jnp.bfloat16
F32 = jnp.float32


def shifted(value, axis, step):
    size = lax.axis_size(axis)
    return lax.ppermute(value, axis, [(i, (i + step) % size) for i in range(size)])


def after(value, *others):
    return lax.optimization_barrier((value, *others))[0]


def to_each(value, axis, groups):
    copies = jnp.broadcast_to(value[None], (len(groups[0]), *value.shape))
    moved = lax.all_to_all(copies, axis, 0, 0, axis_index_groups=groups, tiled=True)
    return moved.reshape(len(groups[0]) * value.shape[0], *value.shape[1:])


def dot(a, b, over_a=1, over_b=0):
    return lax.dot_general(a, b, (((over_a,), (over_b,)), ((), ())), preferred_element_type=F32)


def call(body, outs, flops, aliases=None, smem=(), scratch=()):
    def run(*args):
        specs = [
            pl.BlockSpec(memory_space=pltpu.SMEM if i in smem else pltpu.VMEM)
            for i in range(len(args))
        ]
        many = isinstance(outs, (list, tuple))
        shapes = list(outs) if many else [outs]
        size = sum(math.prod(s.shape) * s.dtype.itemsize for s in (*args, *shapes))
        out_specs = [pl.BlockSpec(memory_space=pltpu.VMEM) for _ in shapes]
        return pl.pallas_call(
            body,
            out_shape=shapes if many else shapes[0],
            in_specs=specs,
            out_specs=out_specs if many else out_specs[0],
            input_output_aliases=aliases or {},
            scratch_shapes=list(scratch),
            compiler_params=pltpu.CompilerParams(vmem_limit_bytes=32 << 20),
            cost_estimate=pl.CostEstimate(flops=flops, bytes_accessed=size, transcendentals=0),
        )(*args)

    return run


def shape(dims, dtype):
    return jax.ShapeDtypeStruct(dims, dtype)


def pack_weights_body(up, bias, down, out):
    hidden, width = up.shape
    out[:hidden, :] = up[...]
    row = bias[...]
    high = row.astype(BF)
    low = (row - high.astype(F32)).astype(BF)
    slab = jnp.concatenate(
        [high.astype(F32), low.astype(F32), jnp.zeros((ROWS - 2, hidden), F32)], axis=0
    )
    slab = jnp.concatenate([slab, jnp.zeros((ROWS, width - hidden), F32)], axis=1)
    out[hidden : hidden + ROWS, :] = slab.astype(BF)
    out[hidden + ROWS :, :] = down[...]


def dispatch_body(number, capacity, ids, gates, tokens, buffer, high, low):
    count = ids.shape[1]
    group = number * ROWS
    name = lax.broadcasted_iota(jnp.int32, (number, count), 0)
    first = (ids[0:1, :] == name).astype(F32)
    second = (ids[1:2, :] == name).astype(F32)
    above = lax.broadcasted_iota(jnp.int32, (count, count), 1)
    earlier = (lax.broadcasted_iota(jnp.int32, (count, count), 0) < above).astype(BF)
    before = dot((first + second).astype(BF), earlier)
    place0 = jnp.sum(before * first, axis=0, keepdims=True).astype(jnp.int32)
    place1 = jnp.sum((before + first) * second, axis=0, keepdims=True).astype(jnp.int32)
    slot0 = ids[0:1, :] * capacity + place0
    slot1 = ids[1:2, :] * capacity + place1
    line = lax.broadcasted_iota(jnp.int32, (4 * group, count), 0)
    part = line // group
    expert = (line % group) // ROWS
    row = line % ROWS
    place = jnp.where(part < 2, part * ROWS + row, 2 * ROWS + row % (ROWS // 2))
    lower = jnp.where(row < ROWS // 2, 2, 3)
    code = jnp.where((part < 2) | (part == lower), expert * capacity + place, -1)
    match0 = jnp.where(slot0 == code, 1.0, 0.0)
    match1 = jnp.where(slot1 == code, 1.0, 0.0)
    table = match0 + match1
    weight = match0 * gates[0:1, :] + match1 * gates[1:2, :]
    top = weight.astype(BF)
    high[...] = top
    low[...] = (weight - top.astype(F32)).astype(BF)
    ends = jnp.concatenate(
        [table[: 2 * group], table[2 * group : 3 * group] + table[3 * group :]], axis=0
    ).astype(BF)
    rows = dot(ends, tokens[...]).astype(BF)
    pack(buffer, rows[:group], rows[group : 2 * group], rows[2 * group :])


def split_of(width):
    return (width // LANES + 1) // 2 * LANES


def pack(buffer, first, second, ends):
    width = first.shape[1]
    cut = split_of(width)
    buffer[:, :width] = first
    buffer[:, width : 2 * width] = second
    row = lax.broadcasted_iota(jnp.int32, (ends.shape[0], 1), 0) % ROWS
    lower = ends[:, :cut].astype(F32)
    upper = jnp.concatenate(
        [ends[:, cut:].astype(F32), jnp.zeros((ends.shape[0], 2 * cut - width), F32)], axis=1
    )
    buffer[:, 2 * width :] = jnp.where(row < ROWS // 2, lower, upper).astype(BF)


def halves(group, half):
    out_row = lax.broadcasted_iota(jnp.int32, (group // 2, group), 0)
    in_row = lax.broadcasted_iota(jnp.int32, (group // 2, group), 1)
    short = ROWS // 2
    return (in_row == out_row // short * ROWS + out_row % short + half * short).astype(BF)


def unpack_body(own, other, rows):
    group = own.shape[0]
    width = rows.shape[1]
    cut = split_of(width)
    base = rows.shape[0] // 2
    for k, ref in enumerate((own, other)):
        at = k * base
        rows[at : at + group, :] = ref[:, :width]
        rows[at + group : at + 2 * group, :] = ref[:, width : 2 * width]
        ends = ref[:, 2 * width :]
        rows[at + 2 * group : at + base, :cut] = dot(halves(group, 0), ends).astype(BF)
        rows[at + 2 * group : at + base, cut:] = dot(
            halves(group, 1), ends[:, : width - cut]
        ).astype(BF)


def contribution(rows, up, bias, down):
    raised = dot(rows, up, 1, 1) + bias
    return dot(jax.nn.gelu(raised).astype(BF), down)


def bias_of(slab):
    return slab[0:1, :].astype(F32) + slab[1:2, :].astype(F32)


def steps_body(pieces, rows, *refs):
    *ins, total, ups, downs = refs
    hidden = (ins[0].shape[0] - ROWS) // 2
    slabs = []
    for k, piece in enumerate(ins[:pieces]):
        at = k * hidden
        ups[at : at + hidden, :] = piece[:hidden, :]
        downs[at : at + hidden, :] = piece[hidden + ROWS :, :]
        slabs.append(bias_of(piece[hidden : hidden + ROWS, :hidden]))
    bias = jnp.concatenate(slabs, axis=1)
    count = rows.shape[0]
    size = count // 4
    for at in range(0, count, size):
        part = contribution(rows[at : at + size, :], ups[...], bias, downs[...])
        if len(ins) > pieces:
            part += ins[pieces][at : at + size, :]
        total[at : at + size, :] = part


def last_body(rows, upper, lower, old, own, other):
    hidden = lower.shape[0]
    total = old[...] + contribution(
        rows[...], upper[:hidden, :], bias_of(upper[hidden:, :hidden]), lower[...]
    )
    half = own.shape[0]
    own[...] = total[:half]
    other[...] = total[half:].astype(BF)


def reduce_body(own, other, bias, buffer):
    group = buffer.shape[0]
    total = (own[...] + other[...].astype(F32) + bias[...]).astype(BF)
    tail = total[2 * group :]
    ends = dot(halves(group, 0), tail, 0, 0) + dot(halves(group, 1), tail, 0, 0)
    pack(buffer, total[:group], total[group : 2 * group], ends.astype(BF))


def combine_body(high, low, buffer, out):
    group = buffer.shape[0]
    width = out.shape[1]
    cut = split_of(width)
    total = None
    for gates in (high, low):
        part = dot(gates[:group, :], buffer[:, :width], 0, 0)
        part += dot(gates[group : 2 * group, :], buffer[:, width : 2 * width], 0, 0)
        lower = dot(gates[2 * group : 3 * group, :], buffer[:, 2 * width :], 0, 0)
        upper = dot(gates[3 * group :, :], buffer[:, 2 * width : 3 * width - cut], 0, 0)
        part += jnp.concatenate([lower, upper], axis=1)
        total = part if total is None else total + part
    out[...] = total.astype(BF)


def select_body(flags, new_keys, new_values, old_keys, old_values, out):
    width, length = new_keys.shape
    block = length // flags.shape[0]
    place = lax.broadcasted_iota(jnp.int32, (width, length), 1) // block
    fresh = jnp.zeros((width, length), jnp.int32)
    for k in range(flags.shape[0]):
        fresh = jnp.where(place == k, flags[k], fresh)
    for k, (new, old) in enumerate(((new_keys, old_keys), (new_values, old_values))):
        chosen = jnp.where(fresh == 1, new[...].astype(F32), old[...].astype(F32))
        out[k * width : (k + 1) * width, :] = chosen.astype(BF)


def attend_body(query, gathered, out):
    width = query.shape[0]
    sources = gathered.shape[0] // (2 * width)
    for head in range(width // HD):
        at = head * HD
        scale = 1.0 / math.sqrt(HD)
        keys = [gathered[2 * width * k + at : 2 * width * k + at + HD, :] for k in range(sources)]
        values = [
            gathered[2 * width * k + width + at : 2 * width * k + width + at + HD, :]
            for k in range(sources)
        ]
        scores = [dot(k, query[at : at + HD, :], 0, 0) * scale for k in keys]
        highest = functools.reduce(
            jnp.maximum, [jnp.max(s, axis=0, keepdims=True) for s in scores]
        )
        totals = mixed = 0.0
        for s, v in zip(scores, values):
            probs = jnp.exp(s - highest)
            totals += jnp.sum(probs, axis=0, keepdims=True)
            mixed += dot(v, probs.astype(BF))
        out[at : at + HD, :] = (mixed / totals).astype(BF)


def local(
    attn_query,
    fresh_keys,
    fresh_values,
    stale_keys,
    stale_values,
    block_flags,
    moe_tokens,
    expert_ids,
    gate_weights,
    up_weight,
    up_bias,
    down_weight,
    down_bias,
):
    width, hidden = up_weight.shape[1:]
    length = attn_query.shape[0]
    tokens_here = moe_tokens.shape[0]
    number = lax.axis_size("seq") * up_weight.shape[0]
    capacity = 5 * tokens_here // (2 * number)
    slots = number * capacity
    group = number * ROWS
    packed = (group, 2 * width + split_of(width))
    ring = lax.axis_size("exp")
    work = 8 * slots * width * hidden

    own_piece = call(
        pack_weights_body, shape((2 * hidden + ROWS, width), BF), 1 << 28
    )(up_weight[0].T, up_bias, down_weight[0])
    passed = [(shifted(own_piece, "exp", 1), shifted(own_piece, "exp", -1))]
    for _ in range(2, ring // 2):
        right, left = passed[-1]
        passed.append((shifted(right, "exp", 1), shifted(left, "exp", -1)))

    own_kv = call(select_body, shape((2 * attn_query.shape[1], length), BF), 1 << 24, smem=(0,))(
        block_flags, fresh_keys.T, fresh_values.T, stale_keys.T, stale_values.T
    )
    size = lax.axis_size("seq")
    near = math.gcd(size, 4)
    far_kv = jnp.concatenate(
        [own_kv] + [shifted(own_kv, "seq", near * k) for k in range(1, size // near)], axis=0
    )

    buffer, high, low = call(
        functools.partial(dispatch_body, number, capacity),
        [shape(packed, BF), shape((4 * group, tokens_here), BF), shape((4 * group, tokens_here), BF)],
        1 << 27,
    )(expert_ids.T, gate_weights.T, moe_tokens)

    def exchanged(value):
        parts = value.reshape(number, ROWS, packed[1])
        moved = lax.all_to_all(parts, "seq", split_axis=0, concat_axis=0, tiled=True)
        return moved.reshape(packed)

    received = exchanged(buffer)
    received = after(received, passed[1])

    runs = [[near * a + b for b in range(near)] for a in range(size // near)]
    gathered = to_each(after(far_kv, received), "seq", runs)

    rows = call(unpack_body, shape((2 * slots, width), BF), 1 << 28)(
        received, shifted(received, "tp", 1)
    )

    def steps(pieces, old=None):
        extra = [] if old is None else [old]
        both = pltpu.VMEM((len(pieces) * hidden, width), BF)
        return call(
            functools.partial(steps_body, len(pieces)),
            shape((2 * slots, width), F32),
            len(pieces) * work,
            aliases={len(pieces) + 1: 0} if extra else None,
            scratch=(both, both),
        )(rows, *pieces, *extra)

    early = steps([own_piece] + [p for pair in passed[:-1] for p in pair])
    total = steps(list(passed[-1]), early)
    right, left = after(passed[-1], early, far_kv)
    upper = shifted(right[: hidden + ROWS], "exp", 1)
    lower = shifted(left[hidden + ROWS :], "exp", -1)
    own, other = call(
        last_body, [shape((slots, width), F32), shape((slots, width), BF)], work
    )(rows, upper, lower, total)
    result = call(reduce_body, shape(packed, BF), 1 << 28)(own, shifted(other, "tp", 1), down_bias)
    back = exchanged(after(result, gathered))
    attn_out = call(attend_body, shape(attn_query.shape[::-1], BF), 1 << 31)(attn_query.T, gathered)
    moe_out = call(combine_body, shape(moe_tokens.shape, BF), 1 << 29)(high, low, back)
    return (attn_out.T, moe_out)


def solution(mesh):
    in_specs = (
        P(("groups", "seq"), ("exp", "tp")),
        P(("groups", "seq"), ("exp", "tp")),
        P(("groups", "seq"), ("exp", "tp")),
        P(("groups", "seq"), ("exp", "tp")),
        P(("groups", "seq"), ("exp", "tp")),
        P(("groups", "seq")),
        P(("groups", "seq", "exp", "tp"), None),
        P(("groups", "seq", "exp", "tp"), None),
        P(("groups", "seq", "exp", "tp"), None),
        P("seq", None, ("exp", "tp")),
        P("seq", ("exp", "tp")),
        P("seq", ("exp", "tp"), None),
        P("seq", None),
    )
    out_specs = (P(("groups", "seq"), ("exp", "tp")), P(("groups", "seq", "exp", "tp"), None))

    return jax.shard_map(local, mesh=mesh, in_specs=in_specs, out_specs=out_specs, check_vma=False)
```

```python
import functools
import math

import jax
import jax.numpy as jnp
from jax import lax
from jax.experimental import pallas as pl
from jax.experimental.pallas import tpu as pltpu
from jax.sharding import PartitionSpec as P


HD = 72
ROWS = 8
LANES = 128
BF = jnp.bfloat16
F32 = jnp.float32


def shifted(value, axis, step):
    size = lax.axis_size(axis)
    return lax.ppermute(value, axis, [(i, (i + step) % size) for i in range(size)])


def after(value, *others):
    return lax.optimization_barrier((value, *others))[0]


def to_each(value, axis, groups):
    copies = jnp.broadcast_to(value[None], (len(groups[0]), *value.shape))
    moved = lax.all_to_all(copies, axis, 0, 0, axis_index_groups=groups, tiled=True)
    return moved.reshape(len(groups[0]) * value.shape[0], *value.shape[1:])


def dot(a, b, over_a=1, over_b=0):
    return lax.dot_general(a, b, (((over_a,), (over_b,)), ((), ())), preferred_element_type=F32)


def call(body, outs, flops, aliases=None, smem=(), scratch=()):
    def run(*args):
        specs = [
            pl.BlockSpec(memory_space=pltpu.SMEM if i in smem else pltpu.VMEM)
            for i in range(len(args))
        ]
        many = isinstance(outs, (list, tuple))
        shapes = list(outs) if many else [outs]
        size = sum(math.prod(s.shape) * s.dtype.itemsize for s in (*args, *shapes))
        out_specs = [pl.BlockSpec(memory_space=pltpu.VMEM) for _ in shapes]
        return pl.pallas_call(
            body,
            out_shape=shapes if many else shapes[0],
            in_specs=specs,
            out_specs=out_specs if many else out_specs[0],
            input_output_aliases=aliases or {},
            scratch_shapes=list(scratch),
            compiler_params=pltpu.CompilerParams(vmem_limit_bytes=32 << 20),
            cost_estimate=pl.CostEstimate(flops=flops, bytes_accessed=size, transcendentals=0),
        )(*args)

    return run


def shape(dims, dtype):
    return jax.ShapeDtypeStruct(dims, dtype)


def pack_weights_body(side, up, bias, down, main, rest):
    hidden, width = up.shape
    half = hidden // 2
    for p in range(2):
        first, second = slice(p * half, (p + 1) * half), slice((1 - p) * half, (2 - p) * half)

        @pl.when(side[0] == p)
        def _(first=first, second=second):
            main[:half, :] = up[first, :]
            main[half:hidden, :] = up[second, :]
            row = jnp.concatenate([bias[:, first], bias[:, second]], axis=1)
            top = row.astype(BF)
            low = (row - top.astype(F32)).astype(BF)
            slab = jnp.concatenate(
                [top.astype(F32), low.astype(F32), jnp.zeros((ROWS - 2, hidden), F32)], axis=0
            )
            slab = jnp.concatenate([slab, jnp.zeros((ROWS, width - hidden), F32)], axis=1)
            main[hidden : hidden + ROWS, :] = slab.astype(BF)
            main[hidden + ROWS :, :] = down[first, :]
            rest[...] = down[second, :]


def dispatch_body(number, capacity, ids, gates, tokens, buffer, high, low):
    count = ids.shape[1]
    group = number * ROWS
    name = lax.broadcasted_iota(jnp.int32, (number, count), 0)
    first = (ids[0:1, :] == name).astype(F32)
    second = (ids[1:2, :] == name).astype(F32)
    above = lax.broadcasted_iota(jnp.int32, (count, count), 1)
    earlier = (lax.broadcasted_iota(jnp.int32, (count, count), 0) < above).astype(BF)
    before = dot((first + second).astype(BF), earlier)
    place0 = jnp.sum(before * first, axis=0, keepdims=True).astype(jnp.int32)
    place1 = jnp.sum((before + first) * second, axis=0, keepdims=True).astype(jnp.int32)
    slot0 = ids[0:1, :] * capacity + place0
    slot1 = ids[1:2, :] * capacity + place1
    line = lax.broadcasted_iota(jnp.int32, (4 * group, count), 0)
    part = line // group
    expert = (line % group) // ROWS
    row = line % ROWS
    place = jnp.where(part < 2, part * ROWS + row, 2 * ROWS + row % (ROWS // 2))
    lower = jnp.where(row < ROWS // 2, 2, 3)
    code = jnp.where((part < 2) | (part == lower), expert * capacity + place, -1)
    match0 = jnp.where(slot0 == code, 1.0, 0.0)
    match1 = jnp.where(slot1 == code, 1.0, 0.0)
    table = match0 + match1
    weight = match0 * gates[0:1, :] + match1 * gates[1:2, :]
    top = weight.astype(BF)
    high[...] = top
    low[...] = (weight - top.astype(F32)).astype(BF)
    ends = jnp.concatenate(
        [table[: 2 * group], table[2 * group : 3 * group] + table[3 * group :]], axis=0
    ).astype(BF)
    rows = dot(ends, tokens[...]).astype(BF)
    pack(buffer, rows[:group], rows[group : 2 * group], rows[2 * group :])


def split_of(width):
    return (width // LANES + 1) // 2 * LANES


def pack(buffer, first, second, ends):
    width = first.shape[1]
    cut = split_of(width)
    buffer[:, :width] = first
    buffer[:, width : 2 * width] = second
    row = lax.broadcasted_iota(jnp.int32, (ends.shape[0], 1), 0) % ROWS
    lower = ends[:, :cut].astype(F32)
    upper = jnp.concatenate(
        [ends[:, cut:].astype(F32), jnp.zeros((ends.shape[0], 2 * cut - width), F32)], axis=1
    )
    buffer[:, 2 * width :] = jnp.where(row < ROWS // 2, lower, upper).astype(BF)


def halves(group, half):
    out_row = lax.broadcasted_iota(jnp.int32, (group // 2, group), 0)
    in_row = lax.broadcasted_iota(jnp.int32, (group // 2, group), 1)
    short = ROWS // 2
    return (in_row == out_row // short * ROWS + out_row % short + half * short).astype(BF)


def unpack_body(own, other, rows):
    group = own.shape[0]
    width = rows.shape[1]
    cut = split_of(width)
    base = rows.shape[0] // 2
    for k, ref in enumerate((own, other)):
        at = k * base
        rows[at : at + group, :] = ref[:, :width]
        rows[at + group : at + 2 * group, :] = ref[:, width : 2 * width]
        ends = ref[:, 2 * width :]
        rows[at + 2 * group : at + base, :cut] = dot(halves(group, 0), ends).astype(BF)
        rows[at + 2 * group : at + base, cut:] = dot(
            halves(group, 1), ends[:, : width - cut]
        ).astype(BF)


def contribution(rows, up, bias, down):
    raised = dot(rows, up, 1, 1) + bias
    return dot(jax.nn.gelu(raised).astype(BF), down)


def bias_of(slab):
    return slab[0:1, :].astype(F32) + slab[1:2, :].astype(F32)


def steps_body(pieces, others, rows, *refs):
    *ins, total, ups, downs = refs
    mains, rests = ins[:pieces], ins[pieces : pieces + others]
    half = (mains[0].shape[0] - ROWS) // 3
    hidden = 2 * half
    slabs = []
    for k, main in enumerate(mains):
        at = k * hidden
        ups[at : at + hidden, :] = main[:hidden, :]
        downs[at : at + half, :] = main[hidden + ROWS :, :]
        slabs.append(bias_of(main[hidden : hidden + ROWS, :hidden]))
    at = half
    for rest in rests:
        for low in range(0, rest.shape[0], half):
            downs[at : at + half, :] = rest[low : low + half, :]
            at += hidden
    bias = jnp.concatenate(slabs, axis=1)
    count = rows.shape[0]
    size = count // 4
    for at in range(0, count, size):
        part = contribution(rows[at : at + size, :], ups[...], bias, downs[...])
        if len(ins) > pieces + others:
            part += ins[-1][at : at + size, :]
        total[at : at + size, :] = part


def last_body(rows, upper, lower, rest, old, own, other, down):
    half = lower.shape[0]
    hidden = 2 * half
    down[:half, :] = lower[...]
    down[half:, :] = rest[...]
    total = old[...] + contribution(
        rows[...], upper[:hidden, :], bias_of(upper[hidden:, :hidden]), down[...]
    )
    count = own.shape[0]
    own[...] = total[:count]
    other[...] = total[count:].astype(BF)


def reduce_body(own, other, bias, buffer):
    group = buffer.shape[0]
    total = (own[...] + other[...].astype(F32) + bias[...]).astype(BF)
    tail = total[2 * group :]
    ends = dot(halves(group, 0), tail, 0, 0) + dot(halves(group, 1), tail, 0, 0)
    pack(buffer, total[:group], total[group : 2 * group], ends.astype(BF))


def combine_body(high, low, buffer, out):
    group = buffer.shape[0]
    width = out.shape[1]
    cut = split_of(width)
    total = None
    for gates in (high, low):
        part = dot(gates[:group, :], buffer[:, :width], 0, 0)
        part += dot(gates[group : 2 * group, :], buffer[:, width : 2 * width], 0, 0)
        lower = dot(gates[2 * group : 3 * group, :], buffer[:, 2 * width :], 0, 0)
        upper = dot(gates[3 * group :, :], buffer[:, 2 * width : 3 * width - cut], 0, 0)
        part += jnp.concatenate([lower, upper], axis=1)
        total = part if total is None else total + part
    out[...] = total.astype(BF)


def select_body(flags, new_keys, new_values, old_keys, old_values, out):
    width, length = new_keys.shape
    block = length // flags.shape[0]
    place = lax.broadcasted_iota(jnp.int32, (width, length), 1) // block
    fresh = jnp.zeros((width, length), jnp.int32)
    for k in range(flags.shape[0]):
        fresh = jnp.where(place == k, flags[k], fresh)
    for k, (new, old) in enumerate(((new_keys, old_keys), (new_values, old_values))):
        chosen = jnp.where(fresh == 1, new[...].astype(F32), old[...].astype(F32))
        out[k * width : (k + 1) * width, :] = chosen.astype(BF)


def attend_body(query, gathered, out):
    width = query.shape[0]
    sources = gathered.shape[0] // (2 * width)
    for head in range(width // HD):
        at = head * HD
        scale = 1.0 / math.sqrt(HD)
        keys = [gathered[2 * width * k + at : 2 * width * k + at + HD, :] for k in range(sources)]
        values = [
            gathered[2 * width * k + width + at : 2 * width * k + width + at + HD, :]
            for k in range(sources)
        ]
        scores = [dot(k, query[at : at + HD, :], 0, 0) * scale for k in keys]
        highest = functools.reduce(
            jnp.maximum, [jnp.max(s, axis=0, keepdims=True) for s in scores]
        )
        totals = mixed = 0.0
        for s, v in zip(scores, values):
            probs = jnp.exp(s - highest)
            totals += jnp.sum(probs, axis=0, keepdims=True)
            mixed += dot(v, probs.astype(BF))
        out[at : at + HD, :] = (mixed / totals).astype(BF)


def local(
    attn_query,
    fresh_keys,
    fresh_values,
    stale_keys,
    stale_values,
    block_flags,
    moe_tokens,
    expert_ids,
    gate_weights,
    up_weight,
    up_bias,
    down_weight,
    down_bias,
):
    width, hidden = up_weight.shape[1:]
    length = attn_query.shape[0]
    tokens_here = moe_tokens.shape[0]
    number = lax.axis_size("seq") * up_weight.shape[0]
    capacity = 5 * tokens_here // (2 * number)
    slots = number * capacity
    group = number * ROWS
    packed = (group, 2 * width + split_of(width))
    ring = lax.axis_size("exp")
    work = 8 * slots * width * hidden

    half = hidden // 2
    side = (lax.axis_index("groups") % 2).astype(jnp.int32).reshape(1)
    own_main, own_rest = call(
        pack_weights_body,
        [shape((hidden + ROWS + half, width), BF), shape((half, width), BF)],
        1 << 24,
        smem=(0,),
    )(side, up_weight[0].T, up_bias, down_weight[0])

    def twin_of(value):
        return lax.ppermute(value, "groups", [(i, i ^ 1) for i in range(lax.axis_size("groups"))])

    passed, rests = [(own_main, own_main)], [own_rest]
    for _ in range(1, ring // 2):
        right, left = passed[-1]
        right, left = shifted(right, "exp", 1), shifted(left, "exp", -1)
        both = jnp.concatenate([right[hidden + ROWS :], left[hidden + ROWS :]], axis=0)
        rests.append(twin_of(both))
        passed.append((right, left))
    lower = shifted(passed[-1][1][hidden + ROWS :], "exp", -1)
    upper = shifted(passed[-1][0][: hidden + ROWS], "exp", 1)
    last_rest = twin_of(lower)

    own_kv = call(select_body, shape((2 * attn_query.shape[1], length), BF), 1 << 24, smem=(0,))(
        block_flags, fresh_keys.T, fresh_values.T, stale_keys.T, stale_values.T
    )
    size = lax.axis_size("seq")
    near = math.gcd(size, 4)
    far_kv = [own_kv] + [shifted(own_kv, "seq", near * k) for k in range(1, size // near)]
    far_kv = jnp.concatenate(far_kv, axis=0)

    buffer, high, low = call(
        functools.partial(dispatch_body, number, capacity),
        [shape(packed, BF), shape((4 * group, tokens_here), BF), shape((4 * group, tokens_here), BF)],
        1 << 27,
    )(expert_ids.T, gate_weights.T, moe_tokens)

    def exchanged(value):
        parts = value.reshape(number, ROWS, packed[1])
        moved = lax.all_to_all(parts, "seq", split_axis=0, concat_axis=0, tiled=True)
        return moved.reshape(packed)

    received = exchanged(buffer)
    received = after(received, passed[2])

    runs = [[near * a + b for b in range(near)] for a in range(size // near)]
    gathered = to_each(after(far_kv, received), "seq", runs)

    rows = call(unpack_body, shape((2 * slots, width), BF), 1 << 28)(
        received, shifted(received, "tp", 1)
    )

    def steps(mains, others, old=None):
        extra = [] if old is None else [old]
        joined = pltpu.VMEM((len(mains) * hidden, width), BF)
        return call(
            functools.partial(steps_body, len(mains), len(others)),
            shape((2 * slots, width), F32),
            len(mains) * work,
            aliases={len(mains) + len(others) + 1: 0} if extra else None,
            scratch=(joined, joined),
        )(rows, *mains, *others, *extra)

    early = steps([own_main] + [p for pair in passed[1:-1] for p in pair], rests[:-1])
    total = steps(list(passed[-1]), rests[-1:], early)
    own, other = call(
        last_body,
        [shape((slots, width), F32), shape((slots, width), BF)],
        work,
        scratch=(pltpu.VMEM((hidden, width), BF),),
    )(rows, upper, lower, last_rest, total)
    result = call(reduce_body, shape(packed, BF), 1 << 28)(own, shifted(other, "tp", 1), down_bias)
    back = exchanged(after(result, gathered))
    attn_out = call(attend_body, shape(attn_query.shape[::-1], BF), 1 << 31)(attn_query.T, gathered)
    moe_out = call(combine_body, shape(moe_tokens.shape, BF), 1 << 29)(high, low, back)
    return (attn_out.T, moe_out)


def solution(mesh):
    in_specs = (
        P(("groups", "seq"), ("exp", "tp")),
        P(("groups", "seq"), ("exp", "tp")),
        P(("groups", "seq"), ("exp", "tp")),
        P(("groups", "seq"), ("exp", "tp")),
        P(("groups", "seq"), ("exp", "tp")),
        P(("groups", "seq")),
        P(("groups", "seq", "exp", "tp"), None),
        P(("groups", "seq", "exp", "tp"), None),
        P(("groups", "seq", "exp", "tp"), None),
        P("seq", None, ("exp", "tp")),
        P("seq", ("exp", "tp")),
        P("seq", ("exp", "tp"), None),
        P("seq", None),
    )
    out_specs = (P(("groups", "seq"), ("exp", "tp")), P(("groups", "seq", "exp", "tp"), None))

    return jax.shard_map(local, mesh=mesh, in_specs=in_specs, out_specs=out_specs, check_vma=False)
```

```python
import functools
import math

import jax
import jax.numpy as jnp
from jax import lax
from jax.experimental import pallas as pl
from jax.experimental.pallas import tpu as pltpu
from jax.sharding import PartitionSpec as P


HD = 72
ROWS = 8
LANES = 128
BF = jnp.bfloat16
F32 = jnp.float32


def shifted(value, axis, step):
    size = lax.axis_size(axis)
    return lax.ppermute(value, axis, [(i, (i + step) % size) for i in range(size)])


def after(value, *others):
    return lax.optimization_barrier((value, *others))[0]


def to_each(value, axis, groups):
    copies = jnp.broadcast_to(value[None], (len(groups[0]), *value.shape))
    moved = lax.all_to_all(copies, axis, 0, 0, axis_index_groups=groups, tiled=True)
    return moved.reshape(len(groups[0]) * value.shape[0], *value.shape[1:])


def dot(a, b, over_a=1, over_b=0):
    return lax.dot_general(a, b, (((over_a,), (over_b,)), ((), ())), preferred_element_type=F32)


def call(body, outs, flops, aliases=None, smem=(), scratch=(), away=()):
    def run(*args):
        specs = [
            pl.BlockSpec(
                memory_space=pltpu.SMEM if i in smem else pl.ANY if i in away else pltpu.VMEM
            )
            for i in range(len(args))
        ]
        many = isinstance(outs, (list, tuple))
        shapes = list(outs) if many else [outs]
        size = sum(math.prod(s.shape) * s.dtype.itemsize for s in (*args, *shapes))
        out_specs = [pl.BlockSpec(memory_space=pl.ANY if away else pltpu.VMEM) for _ in shapes]
        return pl.pallas_call(
            body,
            out_shape=shapes if many else shapes[0],
            in_specs=specs,
            out_specs=out_specs if many else out_specs[0],
            input_output_aliases=aliases or {},
            scratch_shapes=list(scratch),
            compiler_params=pltpu.CompilerParams(vmem_limit_bytes=32 << 20),
            cost_estimate=pl.CostEstimate(flops=flops, bytes_accessed=size, transcendentals=0),
        )(*args)

    return run


def shape(dims, dtype):
    return jax.ShapeDtypeStruct(dims, dtype)


def pack_weights_body(side, up, bias, down, main, rest, slab, sems):
    hidden, width = up.shape
    half = hidden // 2
    for p in range(2):
        first, second = pl.ds(p * half, half), pl.ds((1 - p) * half, half)

        @pl.when(side[0] == p)
        def _(p=p, first=first, second=second):
            moves = [
                pltpu.make_async_copy(up.at[first], main.at[pl.ds(0, half)], sems.at[0]),
                pltpu.make_async_copy(up.at[second], main.at[pl.ds(half, half)], sems.at[1]),
                pltpu.make_async_copy(down.at[first], main.at[pl.ds(hidden + ROWS, half)], sems.at[2]),
                pltpu.make_async_copy(down.at[second], rest, sems.at[3]),
            ]
            for move in moves:
                move.start()
            row = jnp.concatenate(
                [bias[:, p * half : (p + 1) * half], bias[:, (1 - p) * half : (2 - p) * half]], axis=1
            )
            top = row.astype(BF)
            low = (row - top.astype(F32)).astype(BF)
            lines = jnp.concatenate(
                [top.astype(F32), low.astype(F32), jnp.zeros((ROWS - 2, hidden), F32)], axis=0
            )
            lines = jnp.concatenate([lines, jnp.zeros((ROWS, width - hidden), F32)], axis=1)
            slab[...] = lines.astype(BF)
            last = pltpu.make_async_copy(slab, main.at[pl.ds(hidden, ROWS)], sems.at[4])
            last.start()
            for move in moves:
                move.wait()
            last.wait()


def dispatch_body(number, capacity, ids, gates, tokens, buffer, high, low):
    count = ids.shape[1]
    group = number * ROWS
    name = lax.broadcasted_iota(jnp.int32, (number, count), 0)
    first = (ids[0:1, :] == name).astype(F32)
    second = (ids[1:2, :] == name).astype(F32)
    above = lax.broadcasted_iota(jnp.int32, (count, count), 1)
    earlier = (lax.broadcasted_iota(jnp.int32, (count, count), 0) < above).astype(BF)
    before = dot((first + second).astype(BF), earlier)
    place0 = jnp.sum(before * first, axis=0, keepdims=True).astype(jnp.int32)
    place1 = jnp.sum((before + first) * second, axis=0, keepdims=True).astype(jnp.int32)
    slot0 = ids[0:1, :] * capacity + place0
    slot1 = ids[1:2, :] * capacity + place1
    line = lax.broadcasted_iota(jnp.int32, (4 * group, count), 0)
    part = line // group
    expert = (line % group) // ROWS
    row = line % ROWS
    place = jnp.where(part < 2, part * ROWS + row, 2 * ROWS + row % (ROWS // 2))
    lower = jnp.where(row < ROWS // 2, 2, 3)
    code = jnp.where((part < 2) | (part == lower), expert * capacity + place, -1)
    match0 = jnp.where(slot0 == code, 1.0, 0.0)
    match1 = jnp.where(slot1 == code, 1.0, 0.0)
    table = match0 + match1
    weight = match0 * gates[0:1, :] + match1 * gates[1:2, :]
    top = weight.astype(BF)
    high[...] = top
    low[...] = (weight - top.astype(F32)).astype(BF)
    ends = jnp.concatenate(
        [table[: 2 * group], table[2 * group : 3 * group] + table[3 * group :]], axis=0
    ).astype(BF)
    rows = dot(ends, tokens[...]).astype(BF)
    pack(buffer, rows[:group], rows[group : 2 * group], rows[2 * group :])


def split_of(width):
    return (width // LANES + 1) // 2 * LANES


def pack(buffer, first, second, ends):
    width = first.shape[1]
    cut = split_of(width)
    buffer[:, :width] = first
    buffer[:, width : 2 * width] = second
    row = lax.broadcasted_iota(jnp.int32, (ends.shape[0], 1), 0) % ROWS
    lower = ends[:, :cut].astype(F32)
    upper = jnp.concatenate(
        [ends[:, cut:].astype(F32), jnp.zeros((ends.shape[0], 2 * cut - width), F32)], axis=1
    )
    buffer[:, 2 * width :] = jnp.where(row < ROWS // 2, lower, upper).astype(BF)


def halves(group, half):
    out_row = lax.broadcasted_iota(jnp.int32, (group // 2, group), 0)
    in_row = lax.broadcasted_iota(jnp.int32, (group // 2, group), 1)
    short = ROWS // 2
    return (in_row == out_row // short * ROWS + out_row % short + half * short).astype(BF)


def unpack_body(own, other, rows):
    group = own.shape[0]
    width = rows.shape[1]
    cut = split_of(width)
    base = rows.shape[0] // 2
    for k, ref in enumerate((own, other)):
        at = k * base
        rows[at : at + group, :] = ref[:, :width]
        rows[at + group : at + 2 * group, :] = ref[:, width : 2 * width]
        ends = ref[:, 2 * width :]
        rows[at + 2 * group : at + base, :cut] = dot(halves(group, 0), ends).astype(BF)
        rows[at + 2 * group : at + base, cut:] = dot(
            halves(group, 1), ends[:, : width - cut]
        ).astype(BF)


def contribution(rows, up, bias, down):
    raised = dot(rows, up, 1, 1) + bias
    return dot(jax.nn.gelu(raised).astype(BF), down)


def bias_of(slab):
    return slab[0:1, :].astype(F32) + slab[1:2, :].astype(F32)


def steps_body(pieces, others, rows, *refs):
    *ins, total, ups, downs = refs
    mains, rests = ins[:pieces], ins[pieces : pieces + others]
    half = (mains[0].shape[0] - ROWS) // 3
    hidden = 2 * half
    slabs = []
    for k, main in enumerate(mains):
        at = k * hidden
        ups[at : at + hidden, :] = main[:hidden, :]
        downs[at : at + half, :] = main[hidden + ROWS :, :]
        slabs.append(bias_of(main[hidden : hidden + ROWS, :hidden]))
    at = half
    for rest in rests:
        for low in range(0, rest.shape[0], half):
            downs[at : at + half, :] = rest[low : low + half, :]
            at += hidden
    bias = jnp.concatenate(slabs, axis=1)
    count = rows.shape[0]
    size = count // 4
    for at in range(0, count, size):
        part = contribution(rows[at : at + size, :], ups[...], bias, downs[...])
        if len(ins) > pieces + others:
            part += ins[-1][at : at + size, :]
        total[at : at + size, :] = part


def join_body(right, left, out, *upper):
    half = out.shape[0] // 2
    keep = right.shape[0] - half
    out[:half, :] = right[keep:, :]
    out[half:, :] = left[keep:, :]
    for ref in upper:
        ref[...] = right[:keep, :]


def last_body(rows, upper, lower, rest, old, own, other, down):
    half = lower.shape[0]
    hidden = 2 * half
    down[:half, :] = lower[...]
    down[half:, :] = rest[...]
    total = old[...] + contribution(
        rows[...], upper[:hidden, :], bias_of(upper[hidden:, :hidden]), down[...]
    )
    count = own.shape[0]
    own[...] = total[:count]
    other[...] = total[count:].astype(BF)


def reduce_body(own, other, bias, buffer):
    group = buffer.shape[0]
    total = (own[...] + other[...].astype(F32) + bias[...]).astype(BF)
    tail = total[2 * group :]
    ends = dot(halves(group, 0), tail, 0, 0) + dot(halves(group, 1), tail, 0, 0)
    pack(buffer, total[:group], total[group : 2 * group], ends.astype(BF))


def combine_body(high, low, buffer, out):
    group = buffer.shape[0]
    width = out.shape[1]
    cut = split_of(width)
    total = None
    for gates in (high, low):
        part = dot(gates[:group, :], buffer[:, :width], 0, 0)
        part += dot(gates[group : 2 * group, :], buffer[:, width : 2 * width], 0, 0)
        lower = dot(gates[2 * group : 3 * group, :], buffer[:, 2 * width :], 0, 0)
        upper = dot(gates[3 * group :, :], buffer[:, 2 * width : 3 * width - cut], 0, 0)
        part += jnp.concatenate([lower, upper], axis=1)
        total = part if total is None else total + part
    out[...] = total.astype(BF)


def select_body(flags, new_keys, new_values, old_keys, old_values, out):
    width, length = new_keys.shape
    block = length // flags.shape[0]
    place = lax.broadcasted_iota(jnp.int32, (width, length), 1) // block
    fresh = jnp.zeros((width, length), jnp.int32)
    for k in range(flags.shape[0]):
        fresh = jnp.where(place == k, flags[k], fresh)
    for k, (new, old) in enumerate(((new_keys, old_keys), (new_values, old_values))):
        chosen = jnp.where(fresh == 1, new[...].astype(F32), old[...].astype(F32))
        out[k * width : (k + 1) * width, :] = chosen.astype(BF)


def attend_body(query, gathered, out):
    width = query.shape[0]
    sources = gathered.shape[0] // (2 * width)
    for head in range(width // HD):
        at = head * HD
        scale = 1.0 / math.sqrt(HD)
        keys = [gathered[2 * width * k + at : 2 * width * k + at + HD, :] for k in range(sources)]
        values = [
            gathered[2 * width * k + width + at : 2 * width * k + width + at + HD, :]
            for k in range(sources)
        ]
        scores = [dot(k, query[at : at + HD, :], 0, 0) * scale for k in keys]
        highest = functools.reduce(
            jnp.maximum, [jnp.max(s, axis=0, keepdims=True) for s in scores]
        )
        totals = mixed = 0.0
        for s, v in zip(scores, values):
            probs = jnp.exp(s - highest)
            totals += jnp.sum(probs, axis=0, keepdims=True)
            mixed += dot(v, probs.astype(BF))
        out[at : at + HD, :] = (mixed / totals).astype(BF)


def local(
    attn_query,
    fresh_keys,
    fresh_values,
    stale_keys,
    stale_values,
    block_flags,
    moe_tokens,
    expert_ids,
    gate_weights,
    up_weight,
    up_bias,
    down_weight,
    down_bias,
):
    width, hidden = up_weight.shape[1:]
    length = attn_query.shape[0]
    tokens_here = moe_tokens.shape[0]
    number = lax.axis_size("seq") * up_weight.shape[0]
    capacity = 5 * tokens_here // (2 * number)
    slots = number * capacity
    group = number * ROWS
    packed = (group, 2 * width + split_of(width))
    ring = lax.axis_size("exp")
    work = 8 * slots * width * hidden

    half = hidden // 2
    side = (lax.axis_index("groups") % 2).astype(jnp.int32).reshape(1)
    own_main, own_rest = call(
        pack_weights_body,
        [shape((hidden + ROWS + half, width), BF), shape((half, width), BF)],
        1 << 24,
        smem=(0,),
        scratch=(pltpu.VMEM((ROWS, width), BF), pltpu.SemaphoreType.DMA((5,))),
        away=(1, 3),
    )(side, up_weight[0].T, up_bias, down_weight[0])

    def twin_of(value):
        return lax.ppermute(value, "groups", [(i, i ^ 1) for i in range(lax.axis_size("groups"))])

    passed, rests = [(own_main, own_main)], [own_rest]
    for step in range(1, ring // 2):
        right, left = passed[-1]
        right = shifted(right, "exp", 1)
        left = shifted(left, "exp", -1)
        outs = [shape((hidden, width), BF)]
        if step == ring // 2 - 1:
            outs.append(shape((hidden + ROWS, width), BF))
        both, *top = call(join_body, outs, 1 << 20)(right, left)
        rests.append(twin_of(both))
        passed.append((right, left))
    lower = shifted(passed[-1][1][hidden + ROWS :], "exp", -1)
    upper = shifted(top[0], "exp", 1)
    last_rest = twin_of(lower)

    own_kv = call(select_body, shape((2 * attn_query.shape[1], length), BF), 1 << 24, smem=(0,))(
        block_flags, fresh_keys.T, fresh_values.T, stale_keys.T, stale_values.T
    )
    size = lax.axis_size("seq")
    near = math.gcd(size, 4)
    far_kv = [own_kv] + [shifted(own_kv, "seq", near * k) for k in range(1, size // near)]
    far_kv = jnp.concatenate(far_kv, axis=0)

    buffer, high, low = call(
        functools.partial(dispatch_body, number, capacity),
        [shape(packed, BF), shape((4 * group, tokens_here), BF), shape((4 * group, tokens_here), BF)],
        1 << 27,
    )(expert_ids.T, gate_weights.T, moe_tokens)

    def exchanged(value):
        parts = value.reshape(number, ROWS, packed[1])
        moved = lax.all_to_all(parts, "seq", split_axis=0, concat_axis=0, tiled=True)
        return moved.reshape(packed)

    received = exchanged(buffer)
    received = after(received, passed[2])

    runs = [[near * a + b for b in range(near)] for a in range(size // near)]
    gathered = to_each(after(far_kv, received), "seq", runs)

    rows = call(unpack_body, shape((2 * slots, width), BF), 1 << 28)(
        received, shifted(received, "tp", 1)
    )

    def steps(mains, others, old=None):
        extra = [] if old is None else [old]
        joined = pltpu.VMEM((len(mains) * hidden, width), BF)
        return call(
            functools.partial(steps_body, len(mains), len(others)),
            shape((2 * slots, width), F32),
            len(mains) * work,
            aliases={len(mains) + len(others) + 1: 0} if extra else None,
            scratch=(joined, joined),
        )(rows, *mains, *others, *extra)

    early = steps([own_main] + [p for pair in passed[1:-1] for p in pair], rests[:-1])
    total = steps(list(passed[-1]), rests[-1:], early)
    own, other = call(
        last_body,
        [shape((slots, width), F32), shape((slots, width), BF)],
        work,
        scratch=(pltpu.VMEM((hidden, width), BF),),
    )(rows, upper, lower, last_rest, total)
    result = call(reduce_body, shape(packed, BF), 1 << 28)(own, shifted(other, "tp", 1), down_bias)
    back = exchanged(after(result, gathered))
    attn_out = call(attend_body, shape(attn_query.shape[::-1], BF), 1 << 31)(attn_query.T, gathered)
    moe_out = call(combine_body, shape(moe_tokens.shape, BF), 1 << 29)(high, low, back)
    return (attn_out.T, moe_out)


def solution(mesh):
    in_specs = (
        P(("groups", "seq"), ("exp", "tp")),
        P(("groups", "seq"), ("exp", "tp")),
        P(("groups", "seq"), ("exp", "tp")),
        P(("groups", "seq"), ("exp", "tp")),
        P(("groups", "seq"), ("exp", "tp")),
        P(("groups", "seq")),
        P(("groups", "seq", "exp", "tp"), None),
        P(("groups", "seq", "exp", "tp"), None),
        P(("groups", "seq", "exp", "tp"), None),
        P("seq", None, ("exp", "tp")),
        P("seq", ("exp", "tp")),
        P("seq", ("exp", "tp"), None),
        P("seq", None),
    )
    out_specs = (P(("groups", "seq"), ("exp", "tp")), P(("groups", "seq", "exp", "tp"), None))

    return jax.shard_map(local, mesh=mesh, in_specs=in_specs, out_specs=out_specs, check_vma=False)
```
